16 devices in a mesh: dp: 2 (over z), tp: 8 (over y, x, core).
Axes of the slice: x: 2, y: 2, z: 2, core: 2. Of those that a mesh axis runs over, the one named last changes fastest.
Arguments:
- hidden: bfloat16 [4, 512, 2048], P('dp')
- targets: int32 [4, 512], P('dp')
- resp_mask: int32 [4, 512], P('dp')
- old_logp: float32 [4, 512], P('dp')
- advantages: float32 [4, 512], P('dp')
- gain: bfloat16 [2048], replicated
- w_head: bfloat16 [128256, 2048], P('tp')
Outputs:
- output 1: float32 [], replicated
- output 2: bfloat16 [4, 512, 2048], P('dp')
- output 3: float32 [128256, 2048], P(('tp', 'dp'))
- output 4: float32 [2048], replicated
All inputs are finite; a program needn't handle non-finite values.
Results may differ from the reference program's by a relative error of at most 0.001.
Values sent between devices are 32-bit elements.
A program may use at most 1 GiB of HBM per device.

```python
import math
import jax
import jax.numpy as jnp
from jax import lax

ROWS = 4
SEQ = 512
DIM = 2048
VOCAB = 128256
TOK_BLOCK = math.gcd(ROWS * SEQ, 128)
EPSILON = 1e-5
CLIP_LOW = 0.8
CLIP_HIGH = 1.2
DUAL_CLIP = 3.0


def norm_apply(h_rows, gain):
    h_float = h_rows.astype(jnp.float32)
    inv_rms = lax.rsqrt(jnp.mean(h_float * h_float, axis=-1, keepdims=True) + EPSILON)
    unit_rows = h_float * inv_rms
    return unit_rows, inv_rms, (unit_rows * gain.astype(jnp.float32)).astype(jnp.bfloat16)


def token_stats(x_rows, tgt_flat, w_head):
    def one_block(block_args):
        x_block, tgt_block = block_args
        logits = jnp.dot(x_block, w_head.T, preferred_element_type=jnp.float32)
        row_max = jnp.max(logits, axis=-1)
        log_norm = row_max + jnp.log(jnp.sum(jnp.exp(logits - row_max[:, None]), axis=-1))
        is_target = jnp.arange(VOCAB)[None, :] == tgt_block[:, None]
        return log_norm, jnp.sum(jnp.where(is_target, logits, 0.0), axis=-1)
    log_norm, z_target = lax.map(one_block, (x_rows.reshape(-1, TOK_BLOCK, DIM), tgt_flat.reshape(-1, TOK_BLOCK)))
    return log_norm.reshape(-1), z_target.reshape(-1)


def ppo_terms(logp, old_logp, advantages, tok_weight):
    prob_ratio = jnp.exp(logp - old_logp)
    loss_plain = -advantages * prob_ratio
    loss_clip = -advantages * jnp.clip(prob_ratio, CLIP_LOW, CLIP_HIGH)
    loss_max = jnp.maximum(loss_plain, loss_clip)
    dual_on = (advantages < 0) & (loss_max >= -DUAL_CLIP * advantages)
    tok_loss = jnp.where(dual_on, -DUAL_CLIP * advantages, loss_max)
    d_ratio = jnp.where(loss_plain >= loss_clip, -advantages, 0.0)
    d_ratio = jnp.where(dual_on, 0.0, d_ratio)
    return jnp.sum(tok_weight * tok_loss), tok_weight * d_ratio * prob_ratio


def setup_inputs(seed: int = 0) -> dict:
    keys = jax.random.split(jax.random.key(seed), 10)
    hidden = jax.random.normal(keys[0], (ROWS, SEQ, DIM), jnp.float32).astype(jnp.bfloat16)
    gain = (1.0 + 0.3 * jax.random.normal(keys[1], (DIM,), jnp.float32)).astype(jnp.bfloat16)
    w_head = (jax.random.normal(keys[2], (VOCAB, DIM), jnp.float32) * DIM ** -0.5).astype(jnp.bfloat16)
    targets = jax.random.randint(keys[3], (ROWS, SEQ), 0, VOCAB, jnp.int32)
    lengths = jax.random.randint(keys[4], (ROWS,), 0, SEQ + 1, jnp.int32)
    lengths = lengths.at[0].set(SEQ).at[1].set(0)
    starts = jax.random.randint(keys[5], (ROWS,), 0, SEQ + 1 - lengths, jnp.int32)
    position = jnp.arange(SEQ, dtype=jnp.int32)[None, :]
    resp_mask = ((position >= starts[:, None]) & (position < (starts + lengths)[:, None])).astype(jnp.int32)
    advantages = jax.random.normal(keys[6], (ROWS, SEQ), jnp.float32)
    ratio_pick = jax.random.randint(keys[7], (ROWS, SEQ), 0, 6, jnp.int32)
    ratio_table = jnp.log(jnp.array([0.5, 0.9, 1.0, 1.1, 1.5, 4.5], jnp.float32))
    log_ratio = ratio_table[ratio_pick] + jax.random.uniform(keys[8], (ROWS, SEQ), jnp.float32, -0.03, 0.03)
    x_rows = norm_apply(hidden.reshape(ROWS * SEQ, DIM), gain)[2]
    log_norm, z_target = token_stats(x_rows, targets.reshape(-1), w_head)
    old_logp = ((z_target - log_norm).reshape(ROWS, SEQ) - log_ratio).astype(jnp.float32)
    return {'hidden': hidden, 'targets': targets, 'resp_mask': resp_mask, 'old_logp': old_logp, 'advantages': advantages, 'gain': gain, 'w_head': w_head}


def reference(hidden, targets, resp_mask, old_logp, advantages, gain, w_head):
    row_sums = jnp.sum(resp_mask, axis=1).astype(jnp.float32)
    rows_used = jnp.sum((row_sums > 0).astype(jnp.float32))
    tok_weight = (resp_mask.astype(jnp.float32) / jnp.maximum(row_sums, 1.0)[:, None] / rows_used).reshape(-1)
    unit_rows, inv_rms, x_rows = norm_apply(hidden.reshape(ROWS * SEQ, DIM), gain)
    tgt_flat = targets.reshape(-1)
    log_norm, z_target = token_stats(x_rows, tgt_flat, w_head)
    total_loss, d_logp = ppo_terms(z_target - log_norm, old_logp.reshape(-1), advantages.reshape(-1), tok_weight)

    def grad_block(head_acc, block_args):
        x_block, tgt_block, norm_block, dl_block = block_args
        logits = jnp.dot(x_block, w_head.T, preferred_element_type=jnp.float32)
        soft_probs = jnp.exp(logits - norm_block[:, None])
        is_target = (jnp.arange(VOCAB)[None, :] == tgt_block[:, None]).astype(jnp.float32)
        d_logits = (dl_block[:, None] * (is_target - soft_probs)).astype(jnp.bfloat16)
        dx_block = jnp.dot(d_logits, w_head, preferred_element_type=jnp.float32)
        head_acc = head_acc + jnp.dot(d_logits.T, x_block, preferred_element_type=jnp.float32)
        return head_acc, dx_block

    blocks = (x_rows.reshape(-1, TOK_BLOCK, DIM), tgt_flat.reshape(-1, TOK_BLOCK), log_norm.reshape(-1, TOK_BLOCK), d_logp.reshape(-1, TOK_BLOCK))
    d_head, dx_blocks = lax.scan(grad_block, jnp.zeros((VOCAB, DIM), jnp.float32), blocks)
    d_act = dx_blocks.reshape(ROWS * SEQ, DIM)
    d_gain = jnp.sum(d_act * unit_rows, axis=0)
    d_unit = d_act * gain.astype(jnp.float32)
    d_hidden = inv_rms * (d_unit - unit_rows * jnp.mean(d_unit * unit_rows, axis=-1, keepdims=True))
    return total_loss, d_hidden.astype(jnp.bfloat16).reshape(ROWS, SEQ, DIM), d_head, d_gain
```

```python
import jax
import jax.numpy as jnp
from jax import lax
from jax.sharding import PartitionSpec as P

EPSILON = 1e-5
CLIP_LOW = 0.8
CLIP_HIGH = 1.2
DUAL_CLIP = 3.0


def ppo_terms(logp, old_logp, advantages, tok_weight):
    prob_ratio = jnp.exp(logp - old_logp)
    loss_plain = -advantages * prob_ratio
    loss_clip = -advantages * jnp.clip(prob_ratio, CLIP_LOW, CLIP_HIGH)
    loss_max = jnp.maximum(loss_plain, loss_clip)
    dual_on = (advantages < 0) & (loss_max >= -DUAL_CLIP * advantages)
    tok_loss = jnp.where(dual_on, -DUAL_CLIP * advantages, loss_max)
    d_ratio = jnp.where(loss_plain >= loss_clip, -advantages, 0.0)
    d_ratio = jnp.where(dual_on, 0.0, d_ratio)
    return jnp.sum(tok_weight * tok_loss), tok_weight * d_ratio * prob_ratio


def norm_rows(h_float, gain_float):
    inv_rms = lax.rsqrt(jnp.mean(h_float * h_float, axis=-1, keepdims=True) + EPSILON)
    unit_rows = h_float * inv_rms
    return inv_rms, unit_rows, (unit_rows * gain_float).astype(jnp.bfloat16)


def solution(mesh):
    n_dp, n_tp = mesh.shape['dp'], mesh.shape['tp']

    def local_step(hidden, targets, resp_mask, old_logp, advantages, gain, w_shard):
        row_count, seq_len, width = hidden.shape
        v_dev = w_shard.shape[0] // n_dp
        n_tok = row_count * seq_len
        n_all = n_tok * n_dp
        piece = n_tok // n_tp
        dp_i, tp_i = lax.axis_index('dp'), lax.axis_index('tp')
        gain_float = gain.astype(jnp.float32)
        h_flat = hidden.reshape(n_tok, width)

        h_piece = lax.dynamic_slice_in_dim(h_flat, tp_i * piece, piece, 0).astype(jnp.float32)
        h_all = lax.all_gather(h_piece, ('dp', 'tp'), axis=0, tiled=True)
        small = jnp.stack([targets.reshape(n_tok).astype(jnp.float32), resp_mask.reshape(n_tok).astype(jnp.float32),
                           old_logp.reshape(n_tok), advantages.reshape(n_tok)])
        tok_info = lax.all_gather(small, 'dp', axis=1, tiled=True)
        tgt_all = tok_info[0].astype(jnp.int32)
        mask_all, old_all, adv_all = tok_info[1], tok_info[2], tok_info[3]
        row_sums = jnp.sum(mask_all.reshape(n_dp * row_count, seq_len), axis=1)
        rows_used = jnp.sum((row_sums > 0).astype(jnp.float32))
        tok_weight = (mask_all.reshape(n_dp * row_count, seq_len) / jnp.maximum(row_sums, 1.0)[:, None] / rows_used).reshape(n_all)

        x_all = norm_rows(h_all, gain_float)[2]
        w_half = lax.dynamic_slice_in_dim(w_shard, dp_i * v_dev, v_dev, 0)
        v_base = tp_i * (v_dev * n_dp) + dp_i * v_dev
        logits = lax.dot_general(w_half, x_all, (((1,), (1,)), ((), ())), preferred_element_type=jnp.float32)
        loc_max = jnp.max(logits, axis=0)
        is_target = lax.broadcasted_iota(jnp.int32, (v_dev, 1), 0) == (tgt_all - v_base)[None, :]
        loc_sum = jnp.sum(jnp.exp(logits - loc_max[None, :]), axis=0)
        loc_tgt = jnp.sum(jnp.where(is_target, logits, 0.0), axis=0)
        stats = lax.all_gather(jnp.stack([loc_max, loc_sum, loc_tgt]), ('dp', 'tp'), axis=0, tiled=False)
        row_max = jnp.max(stats[:, 0], axis=0)
        log_norm = row_max + jnp.log(jnp.sum(stats[:, 1] * jnp.exp(stats[:, 0] - row_max[None]), axis=0))
        logp = jnp.sum(stats[:, 2], axis=0) - log_norm
        total_loss, d_logp = ppo_terms(logp, old_all, adv_all, tok_weight)

        soft_probs = jnp.exp(logits - log_norm[None, :])
        d_logits = (d_logp[None, :] * (jnp.where(is_target, 1.0, 0.0) - soft_probs)).astype(jnp.bfloat16)
        dx_part = lax.dot_general(d_logits, w_half, (((0,), (0,)), ((), ())), preferred_element_type=jnp.float32)
        dx_mine = lax.psum_scatter(dx_part, ('dp', 'tp'), scatter_dimension=0, tiled=True)
        d_head = lax.dot_general(d_logits, x_all, (((1,), (0,)), ((), ())), preferred_element_type=jnp.float32)
        inv_rms, unit_rows, _ = norm_rows(h_piece, gain_float)
        d_gain = lax.psum(jnp.sum(dx_mine * unit_rows, axis=0), ('dp', 'tp'))
        d_unit = dx_mine * gain_float
        dh_piece = inv_rms * (d_unit - unit_rows * jnp.mean(d_unit * unit_rows, axis=-1, keepdims=True))
        dh = lax.all_gather(dh_piece, 'tp', axis=0, tiled=True)
        d_hidden = (dh + 0.0 * gain_float).astype(jnp.bfloat16)
        return total_loss, d_hidden.reshape(row_count, seq_len, width), d_head, d_gain

    row_spec = P('dp', None)
    return jax.shard_map(local_step, mesh=mesh, in_specs=(P('dp', None, None), row_spec, row_spec, row_spec, row_spec, P(None), P('tp', None)), out_specs=(P(), P('dp', None, None), P(('tp', 'dp'), None), P(None)), check_vma=False)
```

```python
import functools

import jax
import jax.numpy as jnp
from jax import lax
from jax.experimental import pallas as pl
from jax.experimental.pallas import tpu as pltpu
from jax.sharding import PartitionSpec as P

EPSILON = 1e-5
CLIP_LOW = 0.8
CLIP_HIGH = 1.2
DUAL_CLIP = 3.0
MESH = pl.DeviceIdType.MESH
F32, BF16 = jnp.float32, jnp.bfloat16
VMEM_MAX = 67043328
N_CHUNK = 4
V_BLK = 2672
PART_COLS = ((0, 768), (768, 640), (1408, 640))


def ppo_terms(logp, old_logp, advantages, tok_weight):
    prob_ratio = jnp.exp(logp - old_logp)
    loss_plain = -advantages * prob_ratio
    loss_clip = -advantages * jnp.clip(prob_ratio, CLIP_LOW, CLIP_HIGH)
    loss_max = jnp.maximum(loss_plain, loss_clip)
    dual_on = (advantages < 0) & (loss_max >= -DUAL_CLIP * advantages)
    tok_loss = jnp.where(dual_on, -DUAL_CLIP * advantages, loss_max)
    d_ratio = jnp.where(loss_plain >= loss_clip, -advantages, 0.0)
    d_ratio = jnp.where(dual_on, 0.0, d_ratio)
    return jnp.sum(tok_weight * tok_loss), tok_weight * d_ratio * prob_ratio


def norm_rows(h_float, gain_float):
    inv_rms = lax.rsqrt(jnp.mean(h_float * h_float, axis=-1, keepdims=True) + EPSILON)
    unit_rows = h_float * inv_rms
    return inv_rms, unit_rows, (unit_rows * gain_float).astype(BF16)


def logits_kernel(tb, sub, dp_ref, x_ref, w_ref, tgt_ref, z_ref, m_ref, s_ref, t_ref):
    v, t = pl.program_id(0), pl.program_id(1)
    rows = w_ref.shape[0]
    for j in range(tb // sub):
        jc = pl.ds(pl.multiple_of(t * tb + j * sub, sub), sub)
        z = lax.dot_general(w_ref[...], x_ref[j * sub:(j + 1) * sub, :], (((1,), (1,)), ((), ())), preferred_element_type=F32)
        z_ref[:, j * sub:(j + 1) * sub] = z
        z3 = z.reshape(rows // 8, 8, sub)
        m_old = jnp.where(v == 0, -3e38, m_ref[:, jc])
        s_old = jnp.where(v == 0, 0.0, s_ref[:, jc])
        t_old = jnp.where(v == 0, 0.0, t_ref[:, jc])
        m_new = jnp.maximum(m_old, jnp.max(z3, axis=0))
        s_ref[:, jc] = s_old * jnp.exp(m_old - m_new) + jnp.sum(jnp.exp(z3 - m_new[None]), axis=0)
        m_ref[:, jc] = m_new
        hit = lax.broadcasted_iota(jnp.int32, (rows, sub), 0) == tgt_ref[0:1, jc] - v * rows
        t_ref[:, jc] = t_old + jnp.sum(jnp.where(hit, z, 0.0).reshape(rows // 8, 8, sub), axis=0)


def token_logits(x_rows, w_shard, tgt_rel, dp_i, v_dev):
    n_tok, width = x_rows.shape
    tb, n_v = 512, v_dev // V_BLK
    full = pl.BlockSpec((8, n_tok), lambda v, t, d: (0, 0))
    z_t, m, s, zt = pl.pallas_call(
        functools.partial(logits_kernel, tb, 256),
        grid_spec=pltpu.PrefetchScalarGridSpec(
            num_scalar_prefetch=1, grid=(n_v, n_tok // tb),
            in_specs=[pl.BlockSpec((tb, width), lambda v, t, d: (t, 0)),
                      pl.BlockSpec((V_BLK, width), lambda v, t, d: (d[0] * n_v + v, 0)),
                      pl.BlockSpec((1, n_tok), lambda v, t, d: (0, 0))],
            out_specs=[pl.BlockSpec((V_BLK, tb), lambda v, t, d: (v, t)), full, full, full]),
        out_shape=[jax.ShapeDtypeStruct((v_dev, n_tok), F32)] + [jax.ShapeDtypeStruct((8, n_tok), F32)] * 3,
        compiler_params=pltpu.CompilerParams(vmem_limit_bytes=VMEM_MAX),
        cost_estimate=pl.CostEstimate(flops=2 * v_dev * n_tok * width, bytes_accessed=v_dev * n_tok * 4 + v_dev * width * 2, transcendentals=v_dev * n_tok),
    )(dp_i.reshape(1), x_rows, w_shard, tgt_rel)
    m_loc = jnp.max(m, axis=0)
    lse_loc = m_loc + jnp.log(jnp.sum(s * jnp.exp(m - m_loc[None]), axis=0))
    return z_t, lse_loc, jnp.sum(zt, axis=0)


def dx_kernel(v_dev, zo_ref, zr_ref, lse_ref, dl_ref, tgt_ref, w_ref, hp_ref, g_ref, dz_ref, out_ref,
              acc, got0, got1a, got1b, got1c, got2a, got2b, got2c, got3a, got3b, got3c,
              s2a, s2b, s2c, s3a, s3b, s3c, dg, dg_got, snd0, rcv0, snd, rcv, snd_g, rcv_g):
    k, v = pl.program_id(0), pl.program_id(1)
    dp, tp = lax.axis_index('dp'), lax.axis_index('tp')
    core, xx, yy = tp % 2, (tp // 2) % 2, tp // 4
    by_core = (dp, yy * 4 + xx * 2 + (1 - core))
    by_x = (dp, yy * 4 + (1 - xx) * 2 + core)
    by_y = (dp, (1 - yy) * 4 + xx * 2 + core)
    by_z = (1 - dp, tp)
    got1, got2, got3 = (got1a, got1b, got1c), (got2a, got2b, got2c), (got3a, got3b, got3c)
    s2, s3 = (s2a, s2b, s2c), (s3a, s3b, s3c)
    cols = [pl.ds(a, n) for a, n in PART_COLS]
    peers = ((by_z, by_y, by_x), (by_y, by_x, by_z), (by_x, by_z, by_y))

    def copy0(j):
        p = j % 2
        return pltpu.make_async_remote_copy(acc.at[p, 1 - core], got0.at[p], snd0.at[p], rcv0.at[p], device_id=by_core, device_id_type=MESH)

    def copy1(j, part):
        p = j % 2
        src = (acc.at[p, core, 1, :, :, :, cols[0]], acc.at[p, core, :, 1 - yy, :, :, cols[1]], acc.at[p, core, :, :, 1 - xx, :, cols[2]])[part]
        return pltpu.make_async_remote_copy(src, got1[part].at[p], snd.at[0, part, p], rcv.at[0, part, p], device_id=peers[part][0], device_id_type=MESH)

    def copy2(j, part):
        p = j % 2
        src = (s2a.at[1 - yy], s2b.at[:, 1 - xx], s2c.at[1])[part]
        return pltpu.make_async_remote_copy(src, got2[part].at[p], snd.at[1, part, p], rcv.at[1, part, p], device_id=peers[part][1], device_id_type=MESH)

    def copy3(j, part):
        p = j % 2
        src = (s3a.at[1 - xx], s3b.at[1], s3c.at[1 - yy])[part]
        return pltpu.make_async_remote_copy(src, got3[part].at[p], snd.at[2, part, p], rcv.at[2, part, p], device_id=peers[part][2], device_id_type=MESH)

    def stage_a(j):
        copy0(j).wait()
        p = j % 2
        acc[p, core] = acc[p, core] + got0[p]
        for part in range(3):
            copy1(j, part).start()

    def stage_b(j):
        p = j % 2
        for part in range(3):
            copy1(j, part).wait()
        s2a[...] = acc[p, core, 0, :, :, :, cols[0]] + got1a[p]
        s2b[...] = acc[p, core, :, yy, :, :, cols[1]] + got1b[p]
        s2c[...] = acc[p, core, :, :, xx, :, cols[2]] + got1c[p]
        for part in range(3):
            copy2(j, part).start()

    def stage_c(j):
        p = j % 2
        for part in range(3):
            copy2(j, part).wait()
        s3a[...] = s2a[yy] + got2a[p]
        s3b[...] = s2b[:, xx] + got2b[p]
        s3c[...] = s2c[0] + got2c[p]
        for part in range(3):
            copy3(j, part).start()

    def stage_d(j):
        p = j % 2
        for part in range(3):
            copy3(j, part).wait()
        d_act = jnp.concatenate([s3a[xx] + got3a[p], s3b[0] + got3b[p], s3c[yy] + got3c[p]], axis=1)
        rows = pl.ds(pl.multiple_of(j * 32, 32), 32)
        h_rows = hp_ref[rows, :]
        inv_rms = lax.rsqrt(jnp.mean(h_rows * h_rows, axis=-1, keepdims=True) + EPSILON)
        unit_rows = h_rows * inv_rms
        dg[...] += jnp.sum((d_act * unit_rows).reshape(4, 8, d_act.shape[1]), axis=0)
        d_unit = d_act * g_ref[...]
        out_ref[rows, :] = d_unit - unit_rows * jnp.mean(d_unit * unit_rows, axis=-1, keepdims=True)

    @pl.when((k == 0) & (v == 0))
    def _():
        barrier = pltpu.get_barrier_semaphore()
        for peer in (by_core, by_x, by_y, by_z):
            pl.semaphore_signal(barrier, inc=1, device_id=peer, device_id_type=MESH)
        pl.semaphore_wait(barrier, 4)
        dg[...] = jnp.zeros_like(dg)

    @pl.when((k >= 2) & (v == 0))
    def _():
        stage_c(k - 2)

    @pl.when((k >= 1) & (v == 1))
    def _():
        stage_a(k - 1)

    @pl.when((k >= 2) & (v == 1))
    def _():
        stage_d(k - 2)

    @pl.when((k >= 1) & (v == 2))
    def _():
        stage_b(k - 1)

    z = jnp.concatenate([zo_ref[:, 0:128], zr_ref[:, 0:128], zo_ref[:, 128:256], zr_ref[:, 128:256]], axis=1)
    soft = jnp.exp(z - lse_ref[...])
    first = (tp * 2 + dp) * v_dev + v * z.shape[0]
    hit = lax.broadcasted_iota(jnp.int32, z.shape, 0) == tgt_ref[...] - first
    dz = (dl_ref[...] * (jnp.where(hit, 1.0, 0.0) - soft)).astype(BF16)
    dz_ref[...] = dz
    half = w_ref.shape[1] // 2
    for side in range(2):
        c = pl.ds(side * half, half)
        part_dx = lax.dot_general(dz_ref[...], w_ref[:, c], (((0,), (0,)), ((), ())), preferred_element_type=F32)
        acc[k % 2, :, :, :, :, :, c] = jnp.where(v == 0, 0.0, acc[k % 2, :, :, :, :, :, c]) + part_dx.reshape(2, 2, 2, 2, 32, half)

    @pl.when(v == 2)
    def _():
        copy0(k).start()

    @pl.when((k == N_CHUNK - 1) & (v == 2))
    def _():
        stage_c(N_CHUNK - 2)
        stage_a(N_CHUNK - 1)
        stage_d(N_CHUNK - 2)
        stage_b(N_CHUNK - 1)
        stage_c(N_CHUNK - 1)
        stage_d(N_CHUNK - 1)
        last = pltpu.make_async_remote_copy(dg, dg_got, snd_g, rcv_g, device_id=by_z, device_id_type=MESH)
        last.start()
        last.wait()
        out_ref[pl.ds(128, 8), :] = dg[...] + dg_got[...]


def dx_reduced(z_own, z_other, lse, d_logp, tgt, w_shard, h_piece, gain_float, v_dev):
    width = w_shard.shape[1]
    n_all = lse.shape[1]
    tb = n_all // N_CHUNK
    row = pl.BlockSpec((1, tb), lambda k, v: (0, k))
    sizes = [n for _, n in PART_COLS]
    vm = lambda *shape: pltpu.VMEM(shape, F32)
    return pl.pallas_call(
        functools.partial(dx_kernel, v_dev),
        grid=(N_CHUNK, v_dev // V_BLK),
        in_specs=[pl.BlockSpec((V_BLK, tb // 2), lambda k, v: (v, k)), pl.BlockSpec((V_BLK, tb // 2), lambda k, v: (v, k)),
                  row, row, row,
                  pl.BlockSpec((V_BLK, width), lambda k, v: (lax.axis_index('dp') * (v_dev // V_BLK) + v, 0)),
                  pl.BlockSpec(h_piece.shape, lambda k, v: (0, 0), pipeline_mode=pl.Buffered(1)),
                  pl.BlockSpec((1, width), lambda k, v: (0, 0))],
        out_specs=[pl.BlockSpec((V_BLK, tb), lambda k, v: (v, k)), pl.BlockSpec((h_piece.shape[0] + 8, width), lambda k, v: (0, 0), pipeline_mode=pl.Buffered(1))],
        out_shape=[jax.ShapeDtypeStruct((v_dev, n_all), BF16), jax.ShapeDtypeStruct((h_piece.shape[0] + 8, width), F32)],
        scratch_shapes=[vm(2, 2, 2, 2, 2, 32, width), vm(2, 2, 2, 2, 32, width)]
        + [vm(2, 2, 2, 32, n) for n in sizes] + [vm(2, 2, 32, n) for n in sizes] + [vm(2, 32, n) for n in sizes]
        + [vm(2, 2, 32, n) for n in sizes] + [vm(2, 32, n) for n in sizes]
        + [vm(8, width), vm(8, width),
           pltpu.SemaphoreType.DMA((2,)), pltpu.SemaphoreType.DMA((2,)),
           pltpu.SemaphoreType.DMA((3, 3, 2)), pltpu.SemaphoreType.DMA((3, 3, 2)),
           pltpu.SemaphoreType.DMA, pltpu.SemaphoreType.DMA],
        compiler_params=pltpu.CompilerParams(collective_id=0, has_side_effects=True, vmem_limit_bytes=VMEM_MAX),
        cost_estimate=pl.CostEstimate(flops=2 * v_dev * n_all * width, bytes_accessed=v_dev * n_all * 6 + 4 * v_dev * width * 2, transcendentals=v_dev * n_all),
    )(z_own, z_other, lse, d_logp, tgt, w_shard, h_piece, gain_float)


def head_kernel(dz_ref, xo_ref, xr_ref, o_ref, x_all, sem):
    @pl.when(pl.program_id(0) == 0)
    def _():
        copies = [pltpu.make_async_copy(src.at[i], x_all.at[i, z], sem.at[i, z])
                  for i in range(x_all.shape[0]) for z, src in enumerate((xo_ref, xr_ref))]
        for copy in copies:
            copy.start()
        for copy in copies:
            copy.wait()

    o_ref[...] = jnp.dot(dz_ref[...], x_all[...].reshape(dz_ref.shape[1], o_ref.shape[1]), preferred_element_type=F32)


def head_grad(dz, x_own, x_other):
    v_dev, n_all = dz.shape
    width = x_own.shape[1]
    vb, groups = 512, n_all // 256
    return pl.pallas_call(
        head_kernel, grid=(pl.cdiv(v_dev, vb),),
        in_specs=[pl.BlockSpec((vb, n_all), lambda v: (v, 0)), pl.BlockSpec(memory_space=pl.ANY), pl.BlockSpec(memory_space=pl.ANY)],
        out_specs=pl.BlockSpec((vb, width), lambda v: (v, 0)),
        out_shape=jax.ShapeDtypeStruct((v_dev, width), F32),
        scratch_shapes=[pltpu.VMEM((groups, 2, 128, width), BF16), pltpu.SemaphoreType.DMA((groups, 2))],
        compiler_params=pltpu.CompilerParams(vmem_limit_bytes=VMEM_MAX),
        cost_estimate=pl.CostEstimate(flops=2 * v_dev * n_all * width, bytes_accessed=v_dev * width * 4 + v_dev * n_all * 2, transcendentals=0),
    )(dz, x_own.reshape(groups, 128, width), x_other.reshape(groups, 128, width))


def solution(mesh):
    n_dp, n_tp = mesh.shape['dp'], mesh.shape['tp']

    def local_step(hidden, targets, resp_mask, old_logp, advantages, gain, w_shard):
        row_count, seq_len, width = hidden.shape
        v_dev = w_shard.shape[0] // n_dp
        n_tok = row_count * seq_len
        n_all = n_tok * n_dp
        piece = n_tok // n_tp
        dp_i, tp_i = lax.axis_index('dp'), lax.axis_index('tp')
        gain_float = gain.astype(F32)
        h_flat = hidden.reshape(n_tok, width)

        seg = piece // N_CHUNK
        place = (tp_i % 2) * 4 + tp_i // 2
        h_piece = lax.dynamic_index_in_dim(h_flat.reshape(N_CHUNK, n_tp, seg, width), place, 1, keepdims=False).reshape(piece, width).astype(F32)
        h_all = lax.all_gather(h_piece, ('dp', 'tp'), axis=0, tiled=True)

        row_sums = jnp.sum(resp_mask, axis=1).astype(F32)
        used = jnp.sum((row_sums > 0).astype(F32))
        share = (resp_mask.astype(F32) / jnp.maximum(row_sums, 1.0)[:, None]).reshape(n_tok)
        small = jnp.stack([targets.reshape(n_tok).astype(F32), share, old_logp.reshape(n_tok),
                           advantages.reshape(n_tok), jnp.full((n_tok,), used)])
        info = lax.all_gather(small, 'dp', axis=0)
        tgt_abs = info[:, 0].astype(jnp.int32)

        def to_mine(a):
            b = a.reshape(n_dp, 2 * N_CHUNK, 128)
            return jnp.stack([jnp.where(dp_i == 0, b[0], b[1]), jnp.where(dp_i == 0, b[1], b[0])], axis=1).reshape(1, n_all)

        v_base = (tp_i * n_dp + dp_i) * v_dev
        tgt_own = lax.dynamic_index_in_dim(tgt_abs, dp_i, 0, keepdims=True) - v_base
        tgt_other = lax.dynamic_index_in_dim(tgt_abs, 1 - dp_i, 0, keepdims=True) - v_base

        inv_own, _, x_own = norm_rows(h_flat.astype(F32), gain_float)
        x_own = lax.optimization_barrier(x_own)
        z_own, lse_own, zt_own = token_logits(x_own, w_shard, tgt_own, dp_i, v_dev)
        h_all, lse_own, zt_own = lax.optimization_barrier((h_all, lse_own, zt_own))
        h_other = lax.dynamic_index_in_dim(h_all.reshape(n_dp, n_tp // 2, 2, N_CHUNK, seg, width), 1 - dp_i, 0, keepdims=False)
        x_other = norm_rows(h_other, gain_float)[2].transpose(2, 1, 0, 3, 4).reshape(n_tok, width)
        z_other, lse_other, zt_other = token_logits(x_other, w_shard, tgt_other, dp_i, v_dev)

        own_first = dp_i == 0
        mine = jnp.stack([jnp.stack([lse_own, zt_own]), jnp.stack([lse_other, zt_other])])
        mine = jnp.where(own_first, mine, mine[::-1])
        stats = lax.all_gather(mine, ('dp', 'tp'), axis=0, tiled=False)
        lse_max = jnp.max(stats[:, :, 0], axis=0)
        log_norm = lse_max + jnp.log(jnp.sum(jnp.exp(stats[:, :, 0] - lse_max[None]), axis=0))
        logp = jnp.sum(stats[:, :, 1], axis=0) - log_norm
        rows_used = info[0, 4, 0] + info[1, 4, 0]
        total_loss, d_logp = ppo_terms(logp, info[:, 2], info[:, 3], info[:, 1] / rows_used)

        dz, reduced = dx_reduced(z_own, z_other, to_mine(log_norm), to_mine(d_logp), to_mine(tgt_abs), w_shard, h_piece, gain_float[None], v_dev)
        gathered = lax.all_gather(reduced, 'tp', axis=0, tiled=False)
        d_head = head_grad(dz, x_own, x_other)
        d_gain = jnp.sum(gathered[:, piece:], axis=(0, 1))
        d_rows = gathered.reshape(n_tp // 2, 2, piece + 8, width)[:, :, :piece].reshape(n_tp // 2, 2, N_CHUNK, seg, width).transpose(2, 1, 0, 3, 4)
        d_hidden = (d_rows.reshape(n_tok, width) * inv_own).astype(BF16)
        return total_loss, d_hidden.reshape(row_count, seq_len, width), d_head, d_gain

    row_spec = P('dp', None)
    return jax.shard_map(local_step, mesh=mesh, in_specs=(P('dp', None, None), row_spec, row_spec, row_spec, row_spec, P(None), P('tp', None)), out_specs=(P(), P('dp', None, None), P(('tp', 'dp'), None), P(None)), check_vma=False)
```

```python
import functools

import jax
import jax.numpy as jnp
from jax import lax
from jax.experimental import pallas as pl
from jax.experimental.pallas import tpu as pltpu
from jax.sharding import PartitionSpec as P

EPSILON = 1e-5
CLIP_LOW = 0.8
CLIP_HIGH = 1.2
DUAL_CLIP = 3.0
MESH = pl.DeviceIdType.MESH
F32, BF16 = jnp.float32, jnp.bfloat16
VMEM_MAX = 67043328
N_CHUNK = 4
V_BLK = 2672
PART_COLS = ((0, 768), (768, 640), (1408, 640))


def ppo_terms(logp, old_logp, advantages, tok_weight):
    prob_ratio = jnp.exp(logp - old_logp)
    loss_plain = -advantages * prob_ratio
    loss_clip = -advantages * jnp.clip(prob_ratio, CLIP_LOW, CLIP_HIGH)
    loss_max = jnp.maximum(loss_plain, loss_clip)
    dual_on = (advantages < 0) & (loss_max >= -DUAL_CLIP * advantages)
    tok_loss = jnp.where(dual_on, -DUAL_CLIP * advantages, loss_max)
    d_ratio = jnp.where(loss_plain >= loss_clip, -advantages, 0.0)
    d_ratio = jnp.where(dual_on, 0.0, d_ratio)
    return jnp.sum(tok_weight * tok_loss), tok_weight * d_ratio * prob_ratio


def norm_rows(h_float, gain_float):
    inv_rms = lax.rsqrt(jnp.mean(h_float * h_float, axis=-1, keepdims=True) + EPSILON)
    unit_rows = h_float * inv_rms
    return inv_rms, unit_rows, (unit_rows * gain_float).astype(BF16)


def logits_kernel(tb, sub, dp_ref, h_ref, g_ref, w_ref, tgt_ref, z_ref, l_ref, y_ref, x_out, m_ref, s_ref, t_ref, xs, sem):
    v, t = pl.program_id(0), pl.program_id(1)
    rows = w_ref.shape[0]

    def keep(i):
        return pltpu.make_async_copy(xs.at[i], x_out.at[i], sem.at[i])

    @pl.when(v == 0)
    def _():
        for i in range(tb // 128):
            if len(h_ref.shape) == 2:
                h = h_ref[i * 128:(i + 1) * 128, :].astype(F32)
            else:
                h = h_ref[0, :, i % 2, i // 2].reshape(128, h_ref.shape[-1])
            xs[t, i * 128:(i + 1) * 128, :] = norm_rows(h, g_ref[...])[2]
        keep(t).start()

    @pl.when(v == 1)
    def _():
        keep(t).wait()

    for j in range(tb // sub):
        jc = pl.ds(pl.multiple_of(t * tb + j * sub, sub), sub)
        z = lax.dot_general(w_ref[...], xs[t, j * sub:(j + 1) * sub, :], (((1,), (1,)), ((), ())), preferred_element_type=F32)
        z_ref[:, j * sub:(j + 1) * sub] = z
        z3 = z.reshape(rows // 8, 8, sub)
        m_old = jnp.where(v == 0, -3e38, m_ref[:, jc])
        s_old = jnp.where(v == 0, 0.0, s_ref[:, jc])
        t_old = jnp.where(v == 0, 0.0, t_ref[:, jc])
        m_new = jnp.maximum(m_old, jnp.max(z3, axis=0))
        s_ref[:, jc] = s_old * jnp.exp(m_old - m_new) + jnp.sum(jnp.exp(z3 - m_new[None]), axis=0)
        m_ref[:, jc] = m_new
        hit = lax.broadcasted_iota(jnp.int32, (rows, sub), 0) == tgt_ref[0:1, jc] - v * rows
        t_ref[:, jc] = t_old + jnp.sum(jnp.where(hit, z, 0.0).reshape(rows // 8, 8, sub), axis=0)

    @pl.when((v == pl.num_programs(0) - 1) & (t == pl.num_programs(1) - 1))
    def _():
        m = m_ref[...]
        m_loc = jnp.max(m, axis=0, keepdims=True)
        l_ref[...] = m_loc + jnp.log(jnp.sum(s_ref[...] * jnp.exp(m - m_loc), axis=0, keepdims=True))
        y_ref[...] = jnp.sum(t_ref[...], axis=0, keepdims=True)


def token_logits(h_rows, gain_float, w_shard, tgt_rel, dp_i, v_dev):
    n_tok, width = tgt_rel.shape[1], w_shard.shape[1]
    tb, n_v = 512, v_dev // V_BLK
    n_t = n_tok // tb
    full = pl.BlockSpec((1, n_tok), lambda v, t, d: (0, 0))
    if h_rows.ndim == 2:
        h_spec = pl.BlockSpec((tb, width), lambda v, t, d: (jnp.where(v == 0, t, n_t - 1), 0))
    else:
        per = N_CHUNK // n_t
        h_spec = pl.BlockSpec((1, h_rows.shape[1], 2, per, h_rows.shape[4], width), lambda v, t, d: (1 - d[0], 0, 0, jnp.where(v == 0, t, n_t - 1), 0, 0))
    z_t, lse_loc, zt_loc, x_rows = pl.pallas_call(
        functools.partial(logits_kernel, tb, 256),
        grid_spec=pltpu.PrefetchScalarGridSpec(
            num_scalar_prefetch=1, grid=(n_v, n_t),
            in_specs=[h_spec, pl.BlockSpec((1, width), lambda v, t, d: (0, 0)),
                      pl.BlockSpec((V_BLK, width), lambda v, t, d: (d[0] * n_v + v, 0)),
                      pl.BlockSpec((1, n_tok), lambda v, t, d: (0, 0))],
            out_specs=[pl.BlockSpec((V_BLK, tb), lambda v, t, d: (v, t)), full, full, pl.BlockSpec(memory_space=pl.ANY)],
            scratch_shapes=[pltpu.VMEM((8, n_tok), F32)] * 3 + [pltpu.VMEM((n_t, tb, width), BF16), pltpu.SemaphoreType.DMA((n_t,))]),
        out_shape=[jax.ShapeDtypeStruct((v_dev, n_tok), F32)] + [jax.ShapeDtypeStruct((1, n_tok), F32)] * 2 + [jax.ShapeDtypeStruct((n_t, tb, width), BF16)],
        compiler_params=pltpu.CompilerParams(vmem_limit_bytes=VMEM_MAX),
        cost_estimate=pl.CostEstimate(flops=2 * v_dev * n_tok * width, bytes_accessed=v_dev * n_tok * 4 + v_dev * width * 2, transcendentals=v_dev * n_tok),
    )(dp_i.reshape(1), h_rows, gain_float, w_shard, tgt_rel)
    return z_t, lse_loc[0], zt_loc[0], x_rows


def stats_kernel(mine_ref, out_ref, got, snd, rcv):
    dp, tp = lax.axis_index('dp'), lax.axis_index('tp')
    core, xx, yy = tp % 2, (tp // 2) % 2, tp // 4
    me = dp * 8 + tp

    def peer(r):
        flip = lambda a, bit: 1 - a if (r >> bit) & 1 else a
        return (flip(dp, 3), flip(yy, 2) * 4 + flip(xx, 1) * 2 + flip(core, 0))

    barrier = pltpu.get_barrier_semaphore()
    for r in range(1, 16):
        pl.semaphore_signal(barrier, inc=1, device_id=peer(r), device_id_type=MESH)
    pl.semaphore_wait(barrier, 15)
    copies = [pltpu.make_async_remote_copy(mine_ref, got.at[me], snd.at[r], rcv.at[r], device_id=peer(r), device_id_type=MESH) for r in range(1, 16)]
    for copy in copies:
        copy.start()
    got[me] = mine_ref[...]
    for copy in copies:
        copy.wait()
    out_ref[...] = got[...]


def exchange_stats(mine):
    vmem = pl.BlockSpec(memory_space=pltpu.VMEM)
    return pl.pallas_call(
        stats_kernel, in_specs=[vmem], out_specs=vmem,
        out_shape=jax.ShapeDtypeStruct((16,) + mine.shape, F32),
        scratch_shapes=[pltpu.VMEM((16,) + mine.shape, F32), pltpu.SemaphoreType.DMA((16,)), pltpu.SemaphoreType.DMA((16,))],
        compiler_params=pltpu.CompilerParams(collective_id=1, has_side_effects=True),
    )(mine)


def dx_kernel(v_dev, zo_ref, zr_ref, lse_ref, dl_ref, tgt_ref, w_ref, hp_ref, g_ref, dz_ref, out_ref,
              acc, got0, got1a, got1b, got1c, got2a, got2b, got2c, got3a, got3b, got3c,
              s2a, s2b, s2c, s3a, s3b, s3c, dg, dg_got, snd0, rcv0, snd, rcv, snd_g, rcv_g):
    k, v = pl.program_id(0), pl.program_id(1)
    dp, tp = lax.axis_index('dp'), lax.axis_index('tp')
    core, xx, yy = tp % 2, (tp // 2) % 2, tp // 4
    by_core = (dp, yy * 4 + xx * 2 + (1 - core))
    by_x = (dp, yy * 4 + (1 - xx) * 2 + core)
    by_y = (dp, (1 - yy) * 4 + xx * 2 + core)
    by_z = (1 - dp, tp)
    got1, got2, got3 = (got1a, got1b, got1c), (got2a, got2b, got2c), (got3a, got3b, got3c)
    s2, s3 = (s2a, s2b, s2c), (s3a, s3b, s3c)
    cols = [pl.ds(a, n) for a, n in PART_COLS]
    peers = ((by_z, by_y, by_x), (by_y, by_x, by_z), (by_x, by_z, by_y))

    def copy0(j):
        p = j % 2
        return pltpu.make_async_remote_copy(acc.at[p, 1 - core], got0.at[p], snd0.at[p], rcv0.at[p], device_id=by_core, device_id_type=MESH)

    def copy1(j, part):
        p = j % 2
        src = (acc.at[p, core, 1, :, :, :, cols[0]], acc.at[p, core, :, 1 - yy, :, :, cols[1]], acc.at[p, core, :, :, 1 - xx, :, cols[2]])[part]
        return pltpu.make_async_remote_copy(src, got1[part].at[p], snd.at[0, part, p], rcv.at[0, part, p], device_id=peers[part][0], device_id_type=MESH)

    def copy2(j, part):
        p = j % 2
        src = (s2a.at[1 - yy], s2b.at[:, 1 - xx], s2c.at[1])[part]
        return pltpu.make_async_remote_copy(src, got2[part].at[p], snd.at[1, part, p], rcv.at[1, part, p], device_id=peers[part][1], device_id_type=MESH)

    def copy3(j, part):
        p = j % 2
        src = (s3a.at[1 - xx], s3b.at[1], s3c.at[1 - yy])[part]
        return pltpu.make_async_remote_copy(src, got3[part].at[p], snd.at[2, part, p], rcv.at[2, part, p], device_id=peers[part][2], device_id_type=MESH)

    def stage_a(j):
        copy0(j).wait()
        p = j % 2
        acc[p, core] = acc[p, core] + got0[p]
        for part in range(3):
            copy1(j, part).start()

    def stage_b(j):
        p = j % 2
        for part in range(3):
            copy1(j, part).wait()
        s2a[...] = acc[p, core, 0, :, :, :, cols[0]] + got1a[p]
        s2b[...] = acc[p, core, :, yy, :, :, cols[1]] + got1b[p]
        s2c[...] = acc[p, core, :, :, xx, :, cols[2]] + got1c[p]
        for part in range(3):
            copy2(j, part).start()

    def stage_c(j):
        p = j % 2
        for part in range(3):
            copy2(j, part).wait()
        s3a[...] = s2a[yy] + got2a[p]
        s3b[...] = s2b[:, xx] + got2b[p]
        s3c[...] = s2c[0] + got2c[p]
        for part in range(3):
            copy3(j, part).start()

    def stage_d(j):
        p = j % 2
        for part in range(3):
            copy3(j, part).wait()
        d_act = jnp.concatenate([s3a[xx] + got3a[p], s3b[0] + got3b[p], s3c[yy] + got3c[p]], axis=1)
        rows = pl.ds(pl.multiple_of(j * 32, 32), 32)
        h_rows = hp_ref[rows, :]
        inv_rms = lax.rsqrt(jnp.mean(h_rows * h_rows, axis=-1, keepdims=True) + EPSILON)
        unit_rows = h_rows * inv_rms
        dg[...] += jnp.sum((d_act * unit_rows).reshape(4, 8, d_act.shape[1]), axis=0)
        d_unit = d_act * g_ref[...]
        out_ref[pl.ds(pl.multiple_of(j * 40, 8), 32), :] = d_unit - unit_rows * jnp.mean(d_unit * unit_rows, axis=-1, keepdims=True)

    @pl.when((k == 0) & (v == 0))
    def _():
        barrier = pltpu.get_barrier_semaphore()
        for peer in (by_core, by_x, by_y, by_z):
            pl.semaphore_signal(barrier, inc=1, device_id=peer, device_id_type=MESH)
        pl.semaphore_wait(barrier, 4)
        dg[...] = jnp.zeros_like(dg)

    @pl.when((k >= 2) & (v == 0))
    def _():
        stage_c(k - 2)

    @pl.when((k >= 1) & (v == 1))
    def _():
        stage_a(k - 1)

    @pl.when((k >= 2) & (v == 1))
    def _():
        stage_d(k - 2)

    @pl.when((k >= 1) & (v == 2))
    def _():
        stage_b(k - 1)

    z = jnp.concatenate([zo_ref[:, 0:128], zr_ref[:, 0:128], zo_ref[:, 128:256], zr_ref[:, 128:256]], axis=1)
    soft = jnp.exp(z - lse_ref[...])
    first = (tp * 2 + dp) * v_dev + v * z.shape[0]
    hit = lax.broadcasted_iota(jnp.int32, z.shape, 0) == tgt_ref[...] - first
    dz = (dl_ref[...] * (jnp.where(hit, 1.0, 0.0) - soft)).astype(BF16)
    dz_ref[...] = dz
    half = w_ref.shape[1] // 2
    for side in range(2):
        c = pl.ds(side * half, half)
        part_dx = lax.dot_general(dz_ref[...], w_ref[:, c], (((0,), (0,)), ((), ())), preferred_element_type=F32)
        acc[k % 2, :, :, :, :, :, c] = jnp.where(v == 0, 0.0, acc[k % 2, :, :, :, :, :, c]) + part_dx.reshape(2, 2, 2, 2, 32, half)

    @pl.when(v == 2)
    def _():
        copy0(k).start()

    @pl.when((k == N_CHUNK - 1) & (v == 2))
    def _():
        stage_c(N_CHUNK - 2)
        stage_a(N_CHUNK - 1)
        stage_d(N_CHUNK - 2)
        stage_b(N_CHUNK - 1)
        stage_c(N_CHUNK - 1)
        stage_d(N_CHUNK - 1)
        last = pltpu.make_async_remote_copy(dg, dg_got, snd_g, rcv_g, device_id=by_z, device_id_type=MESH)
        last.start()
        last.wait()
        out_ref[pl.ds(N_CHUNK * 40 - 8, 8), :] = dg[...] + dg_got[...]


def dx_reduced(z_own, z_other, lse, d_logp, tgt, w_shard, h_piece, gain_float, v_dev):
    width = w_shard.shape[1]
    n_all = lse.shape[1]
    tb = n_all // N_CHUNK
    row = pl.BlockSpec((1, tb), lambda k, v: (0, k))
    sizes = [n for _, n in PART_COLS]
    vm = lambda *shape: pltpu.VMEM(shape, F32)
    return pl.pallas_call(
        functools.partial(dx_kernel, v_dev),
        grid=(N_CHUNK, v_dev // V_BLK),
        in_specs=[pl.BlockSpec((V_BLK, tb // 2), lambda k, v: (v, k)), pl.BlockSpec((V_BLK, tb // 2), lambda k, v: (v, k)),
                  row, row, row,
                  pl.BlockSpec((V_BLK, width), lambda k, v: (lax.axis_index('dp') * (v_dev // V_BLK) + v, 0)),
                  pl.BlockSpec(h_piece.shape, lambda k, v: (0, 0), pipeline_mode=pl.Buffered(1)),
                  pl.BlockSpec((1, width), lambda k, v: (0, 0))],
        out_specs=[pl.BlockSpec((V_BLK, tb), lambda k, v: (v, k)), pl.BlockSpec((N_CHUNK * 40, width), lambda k, v: (0, 0), pipeline_mode=pl.Buffered(1))],
        out_shape=[jax.ShapeDtypeStruct((v_dev, n_all), BF16), jax.ShapeDtypeStruct((N_CHUNK * 40, width), F32)],
        scratch_shapes=[vm(2, 2, 2, 2, 2, 32, width), vm(2, 2, 2, 2, 32, width)]
        + [vm(2, 2, 2, 32, n) for n in sizes] + [vm(2, 2, 32, n) for n in sizes] + [vm(2, 32, n) for n in sizes]
        + [vm(2, 2, 32, n) for n in sizes] + [vm(2, 32, n) for n in sizes]
        + [vm(8, width), vm(8, width),
           pltpu.SemaphoreType.DMA((2,)), pltpu.SemaphoreType.DMA((2,)),
           pltpu.SemaphoreType.DMA((3, 3, 2)), pltpu.SemaphoreType.DMA((3, 3, 2)),
           pltpu.SemaphoreType.DMA, pltpu.SemaphoreType.DMA],
        compiler_params=pltpu.CompilerParams(collective_id=0, has_side_effects=True, vmem_limit_bytes=VMEM_MAX),
        cost_estimate=pl.CostEstimate(flops=2 * v_dev * n_all * width, bytes_accessed=v_dev * n_all * 6 + 4 * v_dev * width * 2, transcendentals=v_dev * n_all),
    )(z_own, z_other, lse, d_logp, tgt, w_shard, h_piece, gain_float)


def head_kernel(dz_ref, xo_ref, xr_ref, o_ref, x_all, sem):
    @pl.when(pl.program_id(0) == 0)
    def _():
        copies = [pltpu.make_async_copy(src.at[i], x_all.at[i, z], sem.at[i, z])
                  for i in range(x_all.shape[0]) for z, src in enumerate((xo_ref, xr_ref))]
        for copy in copies:
            copy.start()
        for copy in copies:
            copy.wait()

    o_ref[...] = jnp.dot(dz_ref[...], x_all[...].reshape(dz_ref.shape[1], o_ref.shape[1]), preferred_element_type=F32)


def head_grad(dz, x_own, x_other):
    v_dev, n_all = dz.shape
    width = x_own.shape[-1]
    vb, groups = 576, n_all // 256
    return pl.pallas_call(
        head_kernel, grid=(pl.cdiv(v_dev, vb),),
        in_specs=[pl.BlockSpec((vb, n_all), lambda v: (v, 0)), pl.BlockSpec(memory_space=pl.ANY), pl.BlockSpec(memory_space=pl.ANY)],
        out_specs=pl.BlockSpec((vb, width), lambda v: (v, 0)),
        out_shape=jax.ShapeDtypeStruct((v_dev, width), F32),
        scratch_shapes=[pltpu.VMEM((groups, 2, 128, width), BF16), pltpu.SemaphoreType.DMA((groups, 2))],
        compiler_params=pltpu.CompilerParams(vmem_limit_bytes=VMEM_MAX),
        cost_estimate=pl.CostEstimate(flops=2 * v_dev * n_all * width, bytes_accessed=v_dev * width * 4 + v_dev * n_all * 2, transcendentals=0),
    )(dz, x_own.reshape(groups, 128, width), x_other.reshape(groups, 128, width))


def finish_kernel(u_ref, h_ref, dh_ref, dg_ref):
    seg = u_ref.shape[3] - 8
    half = h_ref.shape[0] // 2
    for core in range(2):
        rows = pl.ds(core * half, half)
        h = h_ref[rows, :].astype(F32)
        inv_rms = lax.rsqrt(jnp.mean(h * h, axis=-1, keepdims=True) + EPSILON)
        dh_ref[rows, :] = (u_ref[:, core, 0, :seg].reshape(half, h.shape[1]) * inv_rms).astype(BF16)

    @pl.when(pl.program_id(0) == N_CHUNK - 1)
    def _():
        total = u_ref[0, 0, 0, seg:]
        for i in range(1, u_ref.shape[0] * 2):
            total = total + u_ref[i // 2, i % 2, 0, seg:]
        dg_ref[...] = jnp.sum(total, axis=0, keepdims=True)


def finish(gathered, h_flat):
    n_yx, n_core, n_k, rows, width = gathered.shape
    n_tok = h_flat.shape[0]
    return pl.pallas_call(
        finish_kernel, grid=(n_k,),
        in_specs=[pl.BlockSpec((n_yx, n_core, 1, rows, width), lambda k: (0, 0, k, 0, 0)), pl.BlockSpec((n_tok // n_k, width), lambda k: (k, 0))],
        out_specs=[pl.BlockSpec((n_tok // n_k, width), lambda k: (k, 0)), pl.BlockSpec((1, width), lambda k: (0, 0))],
        out_shape=[jax.ShapeDtypeStruct((n_tok, width), BF16), jax.ShapeDtypeStruct((1, width), F32)],
        compiler_params=pltpu.CompilerParams(vmem_limit_bytes=VMEM_MAX),
    )(gathered, h_flat)


def solution(mesh):
    n_dp, n_tp = mesh.shape['dp'], mesh.shape['tp']

    def local_step(hidden, targets, resp_mask, old_logp, advantages, gain, w_shard):
        row_count, seq_len, width = hidden.shape
        v_dev = w_shard.shape[0] // n_dp
        n_tok = row_count * seq_len
        n_all = n_tok * n_dp
        piece = n_tok // n_tp
        dp_i, tp_i = lax.axis_index('dp'), lax.axis_index('tp')
        gain_float = gain.astype(F32)
        h_flat = hidden.reshape(n_tok, width)

        seg = piece // N_CHUNK
        place = (tp_i % 2) * 4 + tp_i // 2
        h_piece = lax.dynamic_index_in_dim(h_flat.reshape(N_CHUNK, n_tp, seg, width), place, 1, keepdims=False).reshape(piece, width).astype(F32)
        h_all = lax.all_gather(h_piece, ('dp', 'tp'), axis=0, tiled=True)

        row_sums = jnp.sum(resp_mask, axis=1).astype(F32)
        used = jnp.sum((row_sums > 0).astype(F32))
        share = (resp_mask.astype(F32) / jnp.maximum(row_sums, 1.0)[:, None]).reshape(n_tok)
        small = jnp.stack([targets.reshape(n_tok).astype(F32), share, old_logp.reshape(n_tok),
                           advantages.reshape(n_tok), jnp.full((n_tok,), used)])
        info = lax.all_gather(small, 'dp', axis=0)
        tgt_abs = info[:, 0].astype(jnp.int32)

        def to_mine(a):
            b = a.reshape(n_dp, 2 * N_CHUNK, 128)
            return jnp.stack([jnp.where(dp_i == 0, b[0], b[1]), jnp.where(dp_i == 0, b[1], b[0])], axis=1).reshape(1, n_all)

        v_base = (tp_i * n_dp + dp_i) * v_dev
        tgt_own = targets.reshape(1, n_tok) - v_base
        tgt_other = lax.dynamic_index_in_dim(tgt_abs, 1 - dp_i, 0, keepdims=True) - v_base

        z_own, lse_own, zt_own, x_own = token_logits(h_flat, gain_float[None], w_shard, tgt_own, dp_i, v_dev)
        h_all, lse_own, zt_own = lax.optimization_barrier((h_all, lse_own, zt_own))
        z_other, lse_other, zt_other, x_other = token_logits(h_all.reshape(n_dp, n_tp // 2, 2, N_CHUNK, seg, width), gain_float[None], w_shard, tgt_other, dp_i, v_dev)

        own_first = dp_i == 0
        mine = jnp.stack([jnp.stack([lse_own, zt_own]), jnp.stack([lse_other, zt_other])])
        mine = jnp.where(own_first, mine, mine[::-1])
        stats = exchange_stats(mine.reshape(4 * n_tok // 128, 128)).reshape(n_dp * n_tp, 2, 2, n_tok)
        lse_max = jnp.max(stats[:, :, 0], axis=0)
        log_norm = lse_max + jnp.log(jnp.sum(jnp.exp(stats[:, :, 0] - lse_max[None]), axis=0))
        logp = jnp.sum(stats[:, :, 1], axis=0) - log_norm
        rows_used = info[0, 4, 0] + info[1, 4, 0]
        total_loss, d_logp = ppo_terms(logp, info[:, 2], info[:, 3], info[:, 1] / rows_used)

        dz, reduced = dx_reduced(z_own, z_other, to_mine(log_norm), to_mine(d_logp), to_mine(tgt_abs), w_shard, h_piece, gain_float[None], v_dev)
        gathered = lax.all_gather(reduced, 'tp', axis=0, tiled=False)
        d_head = head_grad(dz, x_own, x_other)
        d_hidden, d_gain = finish(gathered.reshape(n_tp // 2, 2, N_CHUNK, seg + 8, width), h_flat)
        return total_loss, d_hidden.reshape(row_count, seq_len, width), d_head, d_gain[0]

    row_spec = P('dp', None)
    return jax.shard_map(local_step, mesh=mesh, in_specs=(P('dp', None, None), row_spec, row_spec, row_spec, row_spec, P(None), P('tp', None)), out_specs=(P(), P('dp', None, None), P(('tp', 'dp'), None), P(None)), check_vma=False)
```
